32 devices in a mesh: fsdp: 8 (over z, y), dp: 4 (over x, core).
Axes of the slice: x: 2, y: 2, z: 4, core: 2. Of those that a mesh axis runs over, the one named last changes fastest.
Arguments:
- hidden_in: bfloat16 [8192, 2048], P(('fsdp', 'dp')), may hold values from -40 to 40
- cotangent: bfloat16 [8192, 2048], P(('fsdp', 'dp')), may hold values from -6 to 6
- segment_ids: int32 [8192], P(('fsdp', 'dp')), may hold values from 0 to 4, as said below
- valid_mask: int32 [8192], P(('fsdp', 'dp')), may hold values from 0 to 1, as said below
- input_norm_gain: bfloat16 [2048], P('fsdp'), may hold values from 0.5 to 1.5
- input_norm_bias: bfloat16 [2048], P('fsdp'), may hold values from -1 to 1
- query_key_value_weight: bfloat16 [2048, 6144], P('fsdp'), may hold values from -0.125 to 0.125
- query_key_value_bias: bfloat16 [6144], P('fsdp'), may hold values from -0.29882812 to 0.29882812
- dense_weight: bfloat16 [2048, 2048], P('fsdp'), may hold values from -1 to 1
- dense_bias: bfloat16 [2048], P('fsdp'), may hold values from -1 to 1
- post_norm_gain: bfloat16 [2048], P('fsdp'), may hold values from 0.5 to 1.5
- post_norm_bias: bfloat16 [2048], P('fsdp'), may hold values from -1 to 1
- expand_weight: bfloat16 [2048, 8192], P('fsdp'), may hold values from -0.125 to 0.125
- expand_bias: bfloat16 [8192], P('fsdp'), may hold values from -1 to 1
- contract_weight: bfloat16 [8192, 2048], P('fsdp'), may hold values from -0.0625 to 0.0625
- contract_bias: bfloat16 [2048], P('fsdp'), may hold values from -1 to 1
Outputs:
- block_output: bfloat16 [8192, 2048], P(('fsdp', 'dp'))
- hidden_gradient: float32 [8192, 2048], P(('fsdp', 'dp'))
- input_norm_gain_gradient: float32 [2048], P('fsdp')
- input_norm_bias_gradient: float32 [2048], P('fsdp')
- query_key_value_weight_gradient: float32 [2048, 6144], P('fsdp')
- query_key_value_bias_gradient: float32 [6144], P('fsdp')
- dense_weight_gradient: float32 [2048, 2048], P('fsdp')
- dense_bias_gradient: float32 [2048], P('fsdp')
- post_norm_gain_gradient: float32 [2048], P('fsdp')
- post_norm_bias_gradient: float32 [2048], P('fsdp')
- expand_weight_gradient: float32 [2048, 8192], P('fsdp')
- expand_bias_gradient: float32 [8192], P('fsdp')
- contract_weight_gradient: float32 [8192, 2048], P('fsdp')
- contract_bias_gradient: float32 [2048], P('fsdp')
- branch_norms: float32 [4], replicated
The draws below stay inside these ranges and needn't reach their ends.
Inputs may be any that keep to these rules, and one draw needn't show every extreme that they name: `segment_ids`: within each device's packed row of 256 tokens the ids never fall and equal ids form one contiguous sequence; the padded tail of a row has an id of its own. `valid_mask`: within each device's packed row the ones come first, followed by fewer than 64 zeros.
All inputs are finite; a program needn't handle non-finite values.
Results may differ from the reference program's by a relative error of at most 0.015.
Values may be sent and summed in bfloat16 or wider, within the bound.
A program may use at most 768 MiB of HBM per device.

```python
import jax
import jax.numpy as jnp
from jax import lax

D = 2048
HEADS = 16
HEAD = 128
FF = 8192
ROT = 32
TOK_DEV = 256
MINSEG = 64
SEGMAX = 256
ROWS = 32
TOKENS = 8192


def packing(key):
    split_keys = jax.random.split(jax.random.fold_in(key, 41), 6)
    most_segments = TOK_DEV // MINSEG
    row_kinds = jax.random.randint(split_keys[0], (ROWS,), 0, 4)
    forced = jax.random.randint(split_keys[1], (), 0, ROWS)
    tail_picks = jax.random.randint(split_keys[2], (ROWS, most_segments), 0, 16)
    narrow = jax.random.randint(split_keys[3], (ROWS, most_segments), 0, (SEGMAX - MINSEG) // 4 + 1)
    widest = jax.random.randint(split_keys[4], (ROWS, most_segments), 0, SEGMAX - MINSEG + 1)
    row_numbers = jnp.arange(ROWS, dtype=jnp.int32)
    lengths = MINSEG + jnp.where(tail_picks < 12, narrow, widest)
    lengths = jnp.where(row_numbers[:, None] == forced, MINSEG, lengths)
    boundary_ends = jnp.cumsum(lengths, axis=1)
    longrow = (row_kinds == 0) & (row_numbers != forced)
    padding = jax.random.randint(split_keys[5], (ROWS,), 1, MINSEG)
    padding = jnp.where(longrow, 0, padding)
    places = jnp.arange(TOK_DEV, dtype=jnp.int32)
    counted = jnp.sum((boundary_ends[:, None, :] <= places[None, :, None]).astype(jnp.int32), axis=2)
    counted = jnp.where(longrow[:, None], 0, counted)
    last_valid = TOK_DEV - padding - 1
    last_id = jnp.sum(jnp.where(places[None, :] == last_valid[:, None], counted, 0), axis=1)
    inside = places[None, :] <= last_valid[:, None]
    segments = jnp.where(inside, counted, (last_id + 1)[:, None])
    return (segments.reshape(-1).astype(jnp.int32), inside.astype(jnp.int32).reshape(-1))


def draw_segment_ids(key, part):
    return packing(key)[0]


def draw_valid_mask(key, part):
    return packing(key)[1]


def draw_hidden_in(key, part):
    split_keys = jax.random.split(jax.random.fold_in(key, 17), 3)
    rank = (jnp.arange(TOKENS, dtype=jnp.int32) // TOK_DEV).astype(jnp.float32) / (ROWS - 1)
    token_scale = 2.0 ** jax.random.uniform(split_keys[1], (TOKENS, 1), minval=-0.5, maxval=0.5)
    column_scale = 2.0 ** jax.random.uniform(split_keys[2], (1, D), minval=-0.5, maxval=0.5)
    noise = jax.random.truncated_normal(split_keys[0], -4.0, 4.0, (TOKENS, D))
    row_scale = 0.5 * 10.0 ** rank
    return (noise * row_scale[:, None] * token_scale * column_scale).astype(jnp.bfloat16)


def strengthened(array, stream_key, source, target, blocks, factor):
    def block_of(position):
        return (jnp.arange(array.shape[position]) // (array.shape[position] // blocks)).reshape((-1,) + (1,) * (array.ndim - 1 - position))

    near = jax.random.permutation(stream_key, blocks)[block_of(target)]
    other_side = (block_of(target) + blocks // 2) % blocks
    return jnp.where((block_of(source) == near) | (block_of(source) == other_side), factor * array, array)


def shard_levels(key, shape, pieces, smallest, largest):
    level, own = 1.0, jax.random.fold_in(key, 6)
    for position, parts in pieces:
        heights = jnp.exp(jax.random.uniform(jax.random.fold_in(own, position), (parts,), jnp.float32, smallest / len(pieces), largest / len(pieces)))
        level = level * jnp.repeat(heights, shape[position] // parts).reshape([-1 if axis == position else 1 for axis in range(len(shape))])
    return level


def normal_values(own_key, dims, scale, limit, shards=(), kind=jnp.bfloat16):
    drawn = jax.random.normal(own_key, dims, jnp.float32) * scale
    if len(shards) > 0:
        drawn = shard_levels(own_key, dims, shards, -0.22, 0.18) * drawn
    return jnp.clip(drawn, min=-limit, max=limit).astype(kind)


def gaussian_with(stream_key, dims, width, most, cuts, heavy, kind=jnp.bfloat16):
    array = width * jax.random.normal(stream_key, dims, jnp.float32)
    if cuts:
        array = array * shard_levels(stream_key, dims, cuts, -0.22, 0.18)
    return jnp.clip(strengthened(array, jax.random.fold_in(stream_key, 3), *heavy), -most, most).astype(kind)


def setup_inputs(seed: int = 0) -> dict:
    key_list = jax.random.split(jax.random.key(seed), 17)
    return {
        "hidden_in": draw_hidden_in(jax.random.fold_in(key_list[16], 71), 0),
        "cotangent": gaussian_with(key_list[1], (TOKENS, D), 1.0, 6.0, ((0, 32),), (0, 1, 32, 2.75)),
        "segment_ids": draw_segment_ids(jax.random.fold_in(key_list[16], 71), 0),
        "valid_mask": draw_valid_mask(jax.random.fold_in(key_list[16], 71), 0),
        "input_norm_gain": jnp.clip(1.0 + 0.1 * jax.random.normal(key_list[4], (D,), jnp.float32), 0.5, 1.5).astype(jnp.bfloat16),
        "input_norm_bias": normal_values(key_list[5], (D,), 0.2, 1.0, ((0, 8),)),
        "query_key_value_weight": normal_values(key_list[6], (D, 3 * D), D ** -0.5, 0.125, ((0, 8),)),
        "query_key_value_bias": normal_values(key_list[7], (3 * D,), 0.05, 0.29882812, ((0, 8),)),
        "dense_weight": normal_values(key_list[8], (D, D), (D // 64) ** -0.5, 1.0, ((0, 8),)),
        "dense_bias": normal_values(key_list[9], (D,), 0.2, 1.0, ((0, 8),)),
        "post_norm_gain": jnp.clip(1.0 + 0.1 * jax.random.normal(key_list[10], (D,), jnp.float32), 0.5, 1.5).astype(jnp.bfloat16),
        "post_norm_bias": normal_values(key_list[11], (D,), 0.2, 1.0, ((0, 8),)),
        "expand_weight": normal_values(key_list[12], (D, FF), D ** -0.5, 0.125, ((0, 8),)),
        "expand_bias": normal_values(key_list[13], (FF,), 0.2, 1.0, ((0, 8),)),
        "contract_weight": normal_values(key_list[14], (FF, D), FF ** -0.5, 0.0625, ((0, 8),)),
        "contract_bias": normal_values(key_list[15], (D,), 0.2, 1.0, ((0, 8),)),
    }


@jax.custom_vjp
def low(v):
    return lax.optimization_barrier(v.astype(jnp.bfloat16)).astype(jnp.float32)

@jax.custom_vjp
def low_back(v):
    return v

def low_keep(v):
    return (low(v), None)

def low_pass(kept, grad):
    return (grad,)

def back_keep(v):
    return (v, None)

def back_low(kept, grad):
    return (low(grad),)
low.defvjp(low_keep, low_pass)
low_back.defvjp(back_keep, back_low)
EPSILON = 1e-05

def matmul(left_side, right_side):
    return jnp.dot(left_side, right_side, precision=lax.Precision.HIGHEST, preferred_element_type=jnp.float32)

def normalize(values):
    centered = values - lax.optimization_barrier(jnp.mean(values, axis=-1, keepdims=True))
    spread = lax.optimization_barrier(jnp.mean(centered * centered, axis=-1, keepdims=True))
    return centered * lax.rsqrt(spread + EPSILON)

def gelu_exact(values):
    return 0.5 * values * (1.0 + lax.erf(values * 0.7071067811865476))

def rotate(values, cosine, sine_part):
    halfway = ROT // 2
    former = values[..., :halfway]
    latter = values[..., halfway:ROT]
    return jnp.concatenate([former * cosine - latter * sine_part, latter * cosine + former * sine_part, values[..., ROT:]], axis=-1)

def row_angles(segment_rows):
    places = jnp.arange(TOK_DEV, dtype=jnp.int32)
    before = jnp.concatenate([jnp.full((ROWS, 1), -1, jnp.int32), segment_rows[:, :-1]], axis=1)
    starts = lax.cummax(jnp.where(segment_rows != before, places[None, :], 0), axis=1)
    offsets = (places[None, :] - starts).astype(jnp.float32)
    frequency = 10000.0 ** (-(jnp.arange(ROT // 2, dtype=jnp.float32) * 2.0) / ROT)
    angle_table = offsets[:, :, None] * frequency[None, None, :]
    return (jnp.cos(angle_table)[:, :, None, :], jnp.sin(angle_table)[:, :, None, :])

def attend(row_parts):
    query_row, key_row, value_row, segment_row = row_parts
    places = jnp.arange(TOK_DEV, dtype=jnp.int32)
    allowed = (segment_row[:, None] == segment_row[None, :]) & (places[None, :] <= places[:, None])
    scaled = low_back(jnp.einsum('qhd,khd->hqk', query_row, key_row, precision=lax.Precision.HIGHEST) * HEAD ** (-0.5))
    masked = jnp.where(allowed[None, :, :], scaled, -1e+30)
    highest = lax.optimization_barrier(jnp.max(masked, axis=-1, keepdims=True))
    exponent = jnp.exp(masked - highest)
    chances = exponent / lax.optimization_barrier(jnp.sum(exponent, axis=-1, keepdims=True))
    return jnp.einsum('hqk,khd->qhd', low(chances), value_row, precision=lax.Precision.HIGHEST)

def reference(hidden_in, cotangent, segment_ids, valid_mask, input_norm_gain, input_norm_bias, query_key_value_weight, query_key_value_bias, dense_weight, dense_bias, post_norm_gain, post_norm_bias, expand_weight, expand_bias, contract_weight, contract_bias):
    inputs = hidden_in.astype(jnp.float32)
    segment_rows = segment_ids.reshape(ROWS, TOK_DEV)
    cosine, sine_part = row_angles(segment_rows)
    mask_float = valid_mask.astype(jnp.float32)

    def forward(layer_input, first_gain, first_shift, joined_matrix, joined_shift, dense_matrix, dense_shift, second_gain, second_shift, expand_matrix, expand_shift, shrink_matrix, shrink_shift):
        normed = normalize(layer_input)
        first_in = low(normed * first_gain + first_shift)
        second_in = low(normed * second_gain + second_shift)
        joined = low_back(matmul(first_in, joined_matrix) + joined_shift)
        heads_shape = (ROWS, TOK_DEV, HEADS, HEAD)
        queries = low(rotate(joined[:, :D].reshape(heads_shape), cosine, sine_part))
        keys_all = low(rotate(joined[:, D:2 * D].reshape(heads_shape), cosine, sine_part))
        values_all = low(joined[:, 2 * D:].reshape(heads_shape))
        mixed = lax.map(jax.checkpoint(attend), (queries, keys_all, values_all, segment_rows))
        mixed = low(low_back(mixed.reshape(TOKENS, D)))
        attention = matmul(mixed, dense_matrix) + dense_shift
        expanded = low_back(matmul(second_in, expand_matrix) + expand_shift)
        activated = low(gelu_exact(expanded))
        feed = matmul(activated, shrink_matrix) + shrink_shift
        return (layer_input + attention + feed, (attention, feed))
    result, pullback, branches = jax.vjp(forward, inputs, input_norm_gain.astype(jnp.float32), input_norm_bias.astype(jnp.float32), query_key_value_weight.astype(jnp.float32), query_key_value_bias.astype(jnp.float32), dense_weight.astype(jnp.float32), dense_bias.astype(jnp.float32), post_norm_gain.astype(jnp.float32), post_norm_bias.astype(jnp.float32), expand_weight.astype(jnp.float32), expand_bias.astype(jnp.float32), contract_weight.astype(jnp.float32), contract_bias.astype(jnp.float32), has_aux=True)
    attention, feed = branches
    grad_out = cotangent.astype(jnp.float32) * mask_float[:, None]
    gradients = pullback(grad_out)

    def squares(values):
        return jnp.sum(mask_float[:, None] * values * values)
    valid_count = jnp.sum(mask_float)
    branch_norms = jnp.sqrt(jnp.stack([squares(inputs), squares(attention), squares(feed), squares(result)]) / (valid_count * D))
    return (result.astype(jnp.bfloat16), gradients[0], gradients[1], gradients[2], gradients[3], gradients[4], gradients[5], gradients[6], gradients[7], gradients[8], gradients[9], gradients[10], gradients[11], gradients[12], branch_norms)
```

```python
import functools

import jax
import jax.numpy as jnp
from jax import lax
from jax.experimental import pallas as pl
from jax.experimental.pallas import tpu as pltpu
from jax.sharding import Mesh
from jax.sharding import PartitionSpec as P

HEADS = 16
HEAD = 128
ROT = 32
EPSILON = 1e-05
SWAP = ((0, 1), (1, 0))


def swap(value, axis):
    return lax.ppermute(value, axis, SWAP)


def normalize(values):
    centered = values - jnp.mean(values, axis=-1, keepdims=True)
    spread = jnp.mean(centered * centered, axis=-1, keepdims=True)
    inverse = lax.rsqrt(spread + EPSILON)
    return centered * inverse, inverse


def plane_gather(own):
    half = own.shape[0] // 2
    beside = swap(own, "px")
    above = swap(own, "fi")
    across = jnp.concatenate([swap(beside[:half], "fi"), swap(above[half:], "px")], axis=0)
    near = [own, beside, above, across]
    far = [swap(block, "pc") for block in near]
    return jnp.concatenate(near + far, axis=0)


def small_gather(own):
    for axis in ("px", "fi", "pc"):
        own = jnp.concatenate([own, swap(own, axis)], axis=0)
    return own


def plane_scatter(partial):
    half = partial.shape[1] // 2
    arrived = swap(partial[4:], "pc")

    def add(a, b):
        return a.astype(jnp.float32) + b.astype(jnp.float32)

    mine = add(partial[:4], arrived).astype(partial.dtype)
    upper, lower = mine[:, :half], mine[:, half:]
    got_upper = swap(jnp.stack([upper[1], upper[3]]), "px")
    got_lower = swap(jnp.stack([lower[2], lower[3]]), "fi")
    pass_upper = add(upper[2], got_upper[1]).astype(partial.dtype)
    pass_lower = add(lower[1], got_lower[1]).astype(partial.dtype)
    final_upper = add(upper[0], got_upper[0]) + swap(pass_upper, "fi").astype(jnp.float32)
    final_lower = add(lower[0], got_lower[0]) + swap(pass_lower, "px").astype(jnp.float32)
    return jnp.concatenate([final_upper, final_lower], axis=0)


def replica_gather(own):
    along = lax.axis_index("px")
    core = lax.axis_index("pc")
    other = swap(own, "px")
    pair = jnp.stack([own, other])
    partner = swap(pair, "pc")
    quad = jnp.stack([pair, partner], axis=1).reshape((4,) + own.shape)
    first = along * 2 + core
    order = [first, first ^ 1, first ^ 2, first ^ 3]
    blank = jnp.zeros_like(quad)
    for position, place in enumerate(order):
        blank = lax.dynamic_update_index_in_dim(blank, quad[position], place, 0)
    return blank


def replica_exchange(blocks):
    return lax.all_to_all(blocks, ("px", "pc"), split_axis=0, concat_axis=0, tiled=False)


def attention_kernel(joined_ref, grad_ref, cos_ref, sin_ref, start_ref, mixed_ref, fused_ref):
    tokens = joined_ref.shape[0]
    heads = grad_ref.shape[1] // HEAD
    scale = HEAD ** (-0.5)
    lane = lax.broadcasted_iota(jnp.int32, (tokens, HEAD), 1)
    row = lax.broadcasted_iota(jnp.int32, (tokens, tokens), 0)
    column = lax.broadcasted_iota(jnp.int32, (tokens, tokens), 1)
    allowed = (column <= row) & (column >= start_ref[...])
    cosine = cos_ref[...]
    sine = sin_ref[...]

    def turned(values):
        return jnp.where(
            lane < ROT // 2, pltpu.roll(values, HEAD - ROT // 2, 1), pltpu.roll(values, ROT // 2, 1)
        )

    def dot(a, b, dims):
        return lax.dot_general(a, b, (dims, ((), ())), preferred_element_type=jnp.float32)

    for head in range(heads):
        spans = [slice((part * heads + head) * HEAD, (part * heads + head + 1) * HEAD) for part in range(3)]
        query = joined_ref[:, spans[0]]
        key = joined_ref[:, spans[1]]
        query = (query * cosine + turned(query) * sine).astype(jnp.bfloat16)
        key = (key * cosine + turned(key) * sine).astype(jnp.bfloat16)
        value = joined_ref[:, spans[2]].astype(jnp.bfloat16)
        here = slice(head * HEAD, (head + 1) * HEAD)
        grad = grad_ref[:, here]
        logits = jnp.where(allowed, dot(query, key, ((1,), (1,))) * scale, -1e30)
        exponent = jnp.exp(logits - jnp.max(logits, axis=-1, keepdims=True))
        chances = exponent * (1.0 / jnp.sum(exponent, axis=-1, keepdims=True))
        chances_low = chances.astype(jnp.bfloat16)
        mixed_ref[:, here] = dot(chances_low, value, ((1,), (0,))).astype(jnp.bfloat16)
        chance_grad = dot(grad, value, ((1,), (1,)))
        inner = jnp.sum(chances * chance_grad, axis=-1, keepdims=True)
        logit_grad = (chances * (chance_grad - inner)).astype(jnp.bfloat16)
        query_grad = dot(logit_grad, key, ((1,), (0,))) * scale
        key_grad = dot(logit_grad, query, ((0,), (0,))) * scale
        value_grad = dot(chances_low, grad, ((0,), (0,)))
        fused_ref[:, spans[0]] = (query_grad * cosine - turned(query_grad) * sine).astype(jnp.bfloat16)
        fused_ref[:, spans[1]] = (key_grad * cosine - turned(key_grad) * sine).astype(jnp.bfloat16)
        fused_ref[:, spans[2]] = value_grad.astype(jnp.bfloat16)


def attention(joined, grad, cosine, sine, starts, tokens):
    total = joined.shape[0]
    rows = total // tokens
    wide = joined.shape[1]
    slim = grad.shape[1]

    def block(width):
        return pl.BlockSpec((tokens, width), lambda r: (r, 0))

    return pl.pallas_call(
        attention_kernel,
        grid=(rows,),
        in_specs=[block(wide), block(slim), block(HEAD), block(HEAD), block(1)],
        out_specs=[block(slim), block(wide)],
        out_shape=[
            jax.ShapeDtypeStruct((total, slim), jnp.bfloat16),
            jax.ShapeDtypeStruct((total, wide), jnp.bfloat16),
        ],
        cost_estimate=pl.CostEstimate(
            flops=total * tokens * slim * 14,
            bytes_accessed=total * (wide * 6 + slim * 4 + HEAD * 8),
            transcendentals=total * tokens * (slim // HEAD),
        ),
    )(joined, grad, cosine, sine, starts)


def token_starts(segment_ids):
    places = jnp.arange(segment_ids.shape[0], dtype=jnp.int32)
    same = segment_ids[:, None] == segment_ids[None, :]
    return jnp.min(jnp.where(same, places[None, :], segment_ids.shape[0]), axis=1)


def rotary_tables(offsets):
    frequency = 10000.0 ** (-(jnp.arange(ROT // 2, dtype=jnp.float32) * 2.0) / ROT)
    angle = offsets.astype(jnp.float32)[:, None] * frequency[None, :]
    cosine, sine = jnp.cos(angle), jnp.sin(angle)
    rest = (offsets.shape[0], HEAD - ROT)
    return (
        jnp.concatenate([cosine, cosine, jnp.ones(rest, jnp.float32)], axis=1),
        jnp.concatenate([-sine, sine, jnp.zeros(rest, jnp.float32)], axis=1),
    )


def per_device(
    minor,
    hidden_in,
    cotangent,
    segment_ids,
    valid_mask,
    input_norm_gain,
    input_norm_bias,
    query_key_value_weight,
    query_key_value_bias,
    dense_weight,
    dense_bias,
    post_norm_gain,
    post_norm_bias,
    expand_weight,
    expand_bias,
    contract_weight,
    contract_bias,
):
    fold = ("fo", "fi") if minor else ("fi", "fo")
    outer = lax.axis_size("fo")
    owners = 2 * outer
    side = lax.axis_index("fi")
    replica = lax.axis_index("px") * 2 + lax.axis_index("pc")
    tokens, features = hidden_in.shape
    units = expand_weight.shape[1]
    rows = expand_weight.shape[0]
    ranks = 8
    block = features // ranks
    chunk = units // (owners * 4)
    wide = units // ranks

    def split_units(value):
        lead = value.shape[:-1]
        value = value.reshape(lead + ((outer, 2) if minor else (2, outer)) + (4, chunk))
        return value if minor else jnp.swapaxes(value, -4, -3)

    def units_of(value, whose):
        value = lax.dynamic_index_in_dim(split_units(value), replica, value.ndim + 1, keepdims=False)
        value = lax.dynamic_index_in_dim(value, whose, value.ndim - 2, keepdims=False)
        return value.reshape(value.shape[:-2] + (wide,))

    def block_index(whose):
        return replica * 2 + whose if minor else whose * 4 + replica

    def heads_of(value, whose):
        lead = value.shape[:-1]
        value = value.reshape(lead + (3, ranks, block))
        value = lax.dynamic_index_in_dim(value, block_index(whose), value.ndim - 2, keepdims=False)
        return value.reshape(lead + (3 * block,))

    def both_sides(own, other):
        return jnp.where(side == 0, jnp.stack([own, other]), jnp.stack([other, own]))

    def gather_rows(value):
        whole = lax.all_gather(value, "fo", axis=0, tiled=False)
        if not minor:
            whole = jnp.swapaxes(whole, 0, 1)
        return whole.reshape(features, value.shape[-1])

    def scatter_rows(partial):
        partial = partial.reshape(((outer, 2) if minor else (2, outer)) + (rows, partial.shape[-1]))
        if not minor:
            partial = jnp.swapaxes(partial, 0, 1)
        owned = lax.psum_scatter(partial, "fo", scatter_dimension=0, tiled=False)
        kept = lax.dynamic_index_in_dim(owned, side, 0, keepdims=False)
        given = lax.dynamic_index_in_dim(owned, 1 - side, 0, keepdims=False)
        return both_sides(kept, swap(given, "fi"))

    members = (
        input_norm_gain,
        input_norm_bias,
        post_norm_gain,
        post_norm_bias,
        dense_bias,
        contract_bias,
        query_key_value_bias,
        expand_bias,
    )
    packed = lax.all_gather(jnp.concatenate(members), fold, axis=0, tiled=False)
    packed = packed.reshape(owners, -1)
    vectors = []
    offset = 0
    for member in members:
        length = member.shape[0]
        vectors.append(packed[:, offset : offset + length].reshape(-1).astype(jnp.float32))
        offset += length
    (
        first_gain,
        first_shift,
        second_gain,
        second_shift,
        dense_shift,
        shrink_shift,
        joined_shift,
        expand_shift,
    ) = vectors

    masked = jnp.where(valid_mask[:, None] > 0, cotangent, jnp.zeros_like(cotangent))
    hidden = plane_gather(hidden_in)
    expand_own = units_of(expand_weight, side)
    expand_pair = both_sides(expand_own, swap(units_of(expand_weight, 1 - side), "fi"))
    expand = gather_rows(expand_pair)
    shrink = lax.all_gather(
        lax.dynamic_index_in_dim(
            contract_weight.reshape(4, chunk, features), replica, 0, keepdims=False
        ),
        "fo",
        axis=0,
        tiled=True,
    )
    joined_own = heads_of(query_key_value_weight, side)
    joined_pair = both_sides(joined_own, swap(heads_of(query_key_value_weight, 1 - side), "fi"))
    joined_weight = gather_rows(joined_pair)
    dense_part = lax.all_gather(
        lax.dynamic_index_in_dim(
            dense_weight.reshape(4, rows // 4, features), replica, 0, keepdims=False
        ),
        "fo",
        axis=0,
        tiled=False,
    )
    group = outer // 4
    dense = replica_exchange(dense_part.reshape(4, group, rows // 4, features))
    dense = jnp.swapaxes(dense, 0, 1).reshape(block, features)
    grad = plane_gather(masked)
    starts = token_starts(segment_ids)
    starts_all = small_gather(starts)
    offsets = jnp.tile(jnp.arange(tokens, dtype=jnp.int32), ranks) - starts_all
    cosine, sine = rotary_tables(offsets)

    normed, _ = normalize(hidden.astype(jnp.float32))
    first_in = (normed * first_gain + first_shift).astype(jnp.bfloat16)
    second_in = (normed * second_gain + second_shift).astype(jnp.bfloat16)

    def product(a, b, left, right):
        return lax.dot_general(a, b, (((left,), (right,)), ((), ())), preferred_element_type=jnp.float32)

    expanded = product(second_in, expand, 1, 0) + units_of(expand_shift, side)
    erf_term = lax.erf(expanded * 0.7071067811865476)
    activated = (0.5 * expanded * (1.0 + erf_term)).astype(jnp.bfloat16)
    feed_part = product(activated, shrink, 1, 0).astype(jnp.bfloat16)
    activated_grad = product(grad, shrink, 1, 1)
    slope = 0.5 * (1.0 + erf_term) + expanded * jnp.exp(-0.5 * expanded * expanded) * 0.3989422804014327
    expand_grad = (activated_grad * slope).astype(jnp.bfloat16)
    shrink_weight_part = product(activated, grad, 0, 0).astype(jnp.bfloat16)
    expand_weight_part = product(second_in, expand_grad, 0, 0).astype(jnp.bfloat16)
    second_grad = product(expand_grad, expand, 1, 1)
    feed = plane_scatter(feed_part.reshape(ranks, tokens, features)) + shrink_shift

    joined = product(first_in, joined_weight, 1, 0) + heads_of(joined_shift, side)
    mixed_grad = product(grad, dense, 1, 1).astype(jnp.bfloat16)
    mixed, joined_grad = attention(joined, mixed_grad, cosine, sine, starts_all[:, None], tokens)
    attention_part = product(mixed, dense, 1, 0).astype(jnp.bfloat16)
    attended = plane_scatter(attention_part.reshape(ranks, tokens, features)) + dense_shift
    dense_weight_part = product(mixed, grad, 0, 0).astype(jnp.bfloat16)
    joined_weight_part = product(first_in, joined_grad, 0, 0).astype(jnp.bfloat16)
    first_grad = product(joined_grad, joined_weight, 1, 1)

    normed_grad_part = (first_grad * first_gain + second_grad * second_gain).astype(jnp.bfloat16)
    normed_grad = plane_scatter(normed_grad_part.reshape(ranks, tokens, features))

    inputs = hidden_in.astype(jnp.float32)
    own_normed, own_inverse = normalize(inputs)
    result = inputs + attended + feed
    hidden_gradient = masked.astype(jnp.float32) + own_inverse * (
        normed_grad
        - jnp.mean(normed_grad, axis=-1, keepdims=True)
        - own_normed * jnp.mean(normed_grad * own_normed, axis=-1, keepdims=True)
    )

    shrink_owned = lax.psum_scatter(
        shrink_weight_part.reshape(outer, chunk, features), "fo", scatter_dimension=0, tiled=False
    )
    shrink_weight_grad = replica_gather(shrink_owned).reshape(contract_weight.shape).astype(jnp.float32)
    expand_owned = replica_gather(scatter_rows(expand_weight_part))
    expand_owned = expand_owned.reshape(4, 2, rows, outer, chunk)
    expand_weight_grad = (
        jnp.transpose(expand_owned, (2, 3, 1, 0, 4) if minor else (2, 1, 3, 0, 4))
        .reshape(rows, units)
        .astype(jnp.float32)
    )
    joined_owned = replica_gather(scatter_rows(joined_weight_part)).reshape(4, 2, rows, 3, block)
    joined_weight_grad = (
        jnp.transpose(joined_owned, (2, 3, 0, 1, 4) if minor else (2, 3, 1, 0, 4))
        .reshape(rows, 3 * features)
        .astype(jnp.float32)
    )
    dense_blocks = jnp.swapaxes(dense_weight_part.reshape(group, 4, rows // 4, features), 0, 1)
    dense_blocks = replica_exchange(dense_blocks).reshape(outer, rows // 4, features)
    dense_owned = lax.psum_scatter(dense_blocks, "fo", scatter_dimension=0, tiled=False)
    dense_weight_grad = replica_gather(dense_owned).reshape(rows, features).astype(jnp.float32)

    mask_float = valid_mask.astype(jnp.float32)[:, None]
    statistics = jnp.stack(
        [
            jnp.sum(mask_float * inputs * inputs),
            jnp.sum(mask_float * attended * attended),
            jnp.sum(mask_float * feed * feed),
            jnp.sum(mask_float * result * result),
            jnp.sum(mask_float),
        ]
    )
    joined_bias_sum = jnp.sum(joined_grad, axis=0, dtype=jnp.float32).reshape(3, 1, block)
    joined_bias_sum = lax.dynamic_update_slice(
        jnp.zeros((3, ranks, block), jnp.float32), joined_bias_sum, (0, block_index(side), 0)
    )
    expand_bias_sum = jnp.sum(expand_grad, axis=0, dtype=jnp.float32).reshape(outer, 1, 1, chunk)
    expand_bias_sum = lax.dynamic_update_slice(
        jnp.zeros((outer, 2, 4, chunk), jnp.float32), expand_bias_sum, (0, side, replica, 0)
    )
    if not minor:
        expand_bias_sum = jnp.swapaxes(expand_bias_sum, 0, 1)
    summed = lax.psum(
        jnp.concatenate(
            [
                jnp.sum(first_grad * normed, axis=0),
                jnp.sum(first_grad, axis=0),
                jnp.sum(second_grad * normed, axis=0),
                jnp.sum(second_grad, axis=0),
                jnp.sum(masked.astype(jnp.float32), axis=0),
                joined_bias_sum.reshape(-1),
                expand_bias_sum.reshape(-1),
                statistics,
            ]
        ),
        ("fo", "fi", "px", "pc"),
    )
    owner = lax.axis_index(fold)

    def owned_part(start, length):
        return lax.dynamic_slice_in_dim(summed, start + owner * (length // owners), length // owners)

    bias_out = owned_part(4 * features, features)
    final = 8 * features + units
    branch_norms = jnp.sqrt(summed[final : final + 4] / (summed[final + 4] * features))
    return (
        result.astype(jnp.bfloat16),
        hidden_gradient,
        owned_part(0, features),
        owned_part(features, features),
        joined_weight_grad,
        owned_part(5 * features, 3 * features),
        dense_weight_grad,
        bias_out,
        owned_part(2 * features, features),
        owned_part(3 * features, features),
        expand_weight_grad,
        owned_part(8 * features, units),
        shrink_weight_grad,
        bias_out,
        branch_norms,
    )


def solution(mesh):
    owners = mesh.shape["fsdp"]
    replicas = mesh.shape["dp"]
    minor = 2048 // owners >= HEAD
    outer = owners // 2
    names = ("fo", "fi", "px", "pc") if minor else ("fi", "fo", "px", "pc")
    sizes = (outer, 2) if minor else (2, outer)
    split = Mesh(mesh.devices.reshape(sizes + (replicas // 2, 2)), names)
    fsdp = names[:2]
    every = names
    matrix = P(fsdp, None)
    vector = P(fsdp)
    in_specs = (
        P(every, None),
        P(every, None),
        P(every),
        P(every),
        vector,
        vector,
        matrix,
        vector,
        matrix,
        vector,
        vector,
        vector,
        matrix,
        vector,
        matrix,
        vector,
    )
    out_specs = (
        P(every, None),
        P(every, None),
        vector,
        vector,
        matrix,
        vector,
        matrix,
        vector,
        vector,
        vector,
        matrix,
        vector,
        matrix,
        vector,
        P(),
    )
    return jax.shard_map(
        functools.partial(per_device, minor),
        mesh=split,
        in_specs=in_specs,
        out_specs=out_specs,
        check_vma=False,
    )
```

```python
import jax
import jax.numpy as jnp
from jax import lax
from jax.experimental import pallas as pl
from jax.experimental.pallas import tpu as pltpu
from jax.sharding import Mesh
from jax.sharding import PartitionSpec as P

HEAD = 128
ROT = 32
EPSILON = 1e-05
SWAP = ((0, 1), (1, 0))


def swap(value, axis):
    return lax.ppermute(value, axis, SWAP)


def total_over(value, axes):
    for axis in axes:
        size = lax.axis_size(axis)
        bit = 1
        while bit < size:
            value = value + lax.ppermute(value, axis, tuple((i, i ^ bit) for i in range(size)))
            bit *= 2
    return value


def normalize(values):
    centered = values - jnp.mean(values, axis=-1, keepdims=True)
    spread = jnp.mean(centered * centered, axis=-1, keepdims=True)
    inverse = lax.rsqrt(spread + EPSILON)
    return centered * inverse, inverse


def plane_gather(own):
    half = own.shape[0] // 2
    beside = swap(own, "px")
    above = swap(own, "fi")
    across = jnp.concatenate([swap(beside[:half], "fi"), swap(above[half:], "px")], axis=0)
    near = [own, beside, above, across]
    far = [swap(block, "pc") for block in near]
    return jnp.concatenate(near + far, axis=0)


def small_gather(own):
    for axis in ("px", "fi", "pc"):
        own = jnp.concatenate([own, swap(own, axis)], axis=0)
    return own


def plane_scatter(partial):
    half = partial.shape[1] // 2
    arrived = swap(partial[4:], "pc")

    def add(a, b):
        return a.astype(jnp.float32) + b.astype(jnp.float32)

    mine = add(partial[:4], arrived).astype(partial.dtype)
    upper, lower = mine[:, :half], mine[:, half:]
    got_upper = swap(jnp.stack([upper[1], upper[3]]), "px")
    got_lower = swap(jnp.stack([lower[2], lower[3]]), "fi")
    pass_upper = add(upper[2], got_upper[1]).astype(partial.dtype)
    pass_lower = add(lower[1], got_lower[1]).astype(partial.dtype)
    final_upper = add(upper[0], got_upper[0]) + swap(pass_upper, "fi").astype(jnp.float32)
    final_lower = add(lower[0], got_lower[0]) + swap(pass_lower, "px").astype(jnp.float32)
    return jnp.concatenate([final_upper, final_lower], axis=0)


def replica_gather(own):
    along = lax.axis_index("px")
    core = lax.axis_index("pc")
    other = swap(own, "px")
    pair = jnp.stack([own, other])
    partner = swap(pair, "pc")
    quad = jnp.stack([pair, partner], axis=1).reshape((4,) + own.shape)
    first = along * 2 + core
    order = [first, first ^ 1, first ^ 2, first ^ 3]
    blank = jnp.zeros_like(quad)
    for position, place in enumerate(order):
        blank = lax.dynamic_update_index_in_dim(blank, quad[position], place, 0)
    return blank


def replica_exchange(blocks):
    return lax.all_to_all(blocks, ("px", "pc"), split_axis=0, concat_axis=0, tiled=False)


def attention_kernel(joined_ref, grad_ref, cos_ref, sin_ref, start_ref, mixed_ref, fused_ref):
    tokens = joined_ref.shape[0]
    heads = grad_ref.shape[1] // HEAD
    scale = HEAD ** (-0.5)
    lane = lax.broadcasted_iota(jnp.int32, (tokens, HEAD), 1)
    row = lax.broadcasted_iota(jnp.int32, (tokens, tokens), 0)
    column = lax.broadcasted_iota(jnp.int32, (tokens, tokens), 1)
    allowed = (column <= row) & (column >= start_ref[...])
    cosine = cos_ref[...]
    sine = sin_ref[...]

    def turned(values):
        return jnp.where(
            lane < ROT // 2, pltpu.roll(values, HEAD - ROT // 2, 1), pltpu.roll(values, ROT // 2, 1)
        )

    def dot(a, b, dims):
        return lax.dot_general(a, b, (dims, ((), ())), preferred_element_type=jnp.float32)

    for head in range(heads):
        spans = [slice((part * heads + head) * HEAD, (part * heads + head + 1) * HEAD) for part in range(3)]
        query = joined_ref[:, spans[0]]
        key = joined_ref[:, spans[1]]
        query = (query * cosine + turned(query) * sine).astype(jnp.bfloat16)
        key = (key * cosine + turned(key) * sine).astype(jnp.bfloat16)
        value = joined_ref[:, spans[2]].astype(jnp.bfloat16)
        here = slice(head * HEAD, (head + 1) * HEAD)
        grad = grad_ref[:, here]
        logits = jnp.where(allowed, dot(query, key, ((1,), (1,))) * scale, -1e30)
        exponent = jnp.exp(logits - jnp.max(logits, axis=-1, keepdims=True))
        chances = exponent * (1.0 / jnp.sum(exponent, axis=-1, keepdims=True))
        chances_low = chances.astype(jnp.bfloat16)
        mixed_ref[:, here] = dot(chances_low, value, ((1,), (0,))).astype(jnp.bfloat16)
        chance_grad = dot(grad, value, ((1,), (1,)))
        inner = jnp.sum(chances * chance_grad, axis=-1, keepdims=True)
        logit_grad = (chances * (chance_grad - inner)).astype(jnp.bfloat16)
        query_grad = dot(logit_grad, key, ((1,), (0,))) * scale
        key_grad = dot(logit_grad, query, ((0,), (0,))) * scale
        value_grad = dot(chances_low, grad, ((0,), (0,)))
        fused_ref[:, spans[0]] = (query_grad * cosine - turned(query_grad) * sine).astype(jnp.bfloat16)
        fused_ref[:, spans[1]] = (key_grad * cosine - turned(key_grad) * sine).astype(jnp.bfloat16)
        fused_ref[:, spans[2]] = value_grad.astype(jnp.bfloat16)


def attention(joined, grad, cosine, sine, starts, tokens):
    total = joined.shape[0]
    rows = total // tokens
    wide = joined.shape[1]
    slim = grad.shape[1]

    def block(width):
        return pl.BlockSpec((tokens, width), lambda r: (r, 0))

    return pl.pallas_call(
        attention_kernel,
        grid=(rows,),
        in_specs=[block(wide), block(slim), block(HEAD), block(HEAD), block(1)],
        out_specs=[block(slim), block(wide)],
        out_shape=[
            jax.ShapeDtypeStruct((total, slim), jnp.bfloat16),
            jax.ShapeDtypeStruct((total, wide), jnp.bfloat16),
        ],
        cost_estimate=pl.CostEstimate(
            flops=total * tokens * slim * 14,
            bytes_accessed=total * (wide * 6 + slim * 4 + HEAD * 8),
            transcendentals=total * tokens * (slim // HEAD),
        ),
    )(joined, grad, cosine, sine, starts)


def token_starts(segment_ids):
    places = jnp.arange(segment_ids.shape[0], dtype=jnp.int32)
    same = segment_ids[:, None] == segment_ids[None, :]
    return jnp.min(jnp.where(same, places[None, :], segment_ids.shape[0]), axis=1)


def rotary_tables(offsets):
    frequency = 10000.0 ** (-(jnp.arange(ROT // 2, dtype=jnp.float32) * 2.0) / ROT)
    angle = offsets.astype(jnp.float32)[:, None] * frequency[None, :]
    cosine, sine = jnp.cos(angle), jnp.sin(angle)
    rest = (offsets.shape[0], HEAD - ROT)
    return (
        jnp.concatenate([cosine, cosine, jnp.ones(rest, jnp.float32)], axis=1),
        jnp.concatenate([-sine, sine, jnp.zeros(rest, jnp.float32)], axis=1),
    )


def per_device(
    minor,
    hidden_in,
    cotangent,
    segment_ids,
    valid_mask,
    input_norm_gain,
    input_norm_bias,
    query_key_value_weight,
    query_key_value_bias,
    dense_weight,
    dense_bias,
    post_norm_gain,
    post_norm_bias,
    expand_weight,
    expand_bias,
    contract_weight,
    contract_bias,
):
    fold = ("fo", "fi") if minor else ("fi", "fo")
    outer = lax.axis_size("fo")
    owners = 2 * outer
    side = lax.axis_index("fi")
    replica = lax.axis_index("px") * 2 + lax.axis_index("pc")
    tokens, features = hidden_in.shape
    units = expand_weight.shape[1]
    rows = expand_weight.shape[0]
    ranks = 8
    block = features // ranks
    chunk = units // (owners * 4)
    wide = units // ranks

    def split_units(value):
        lead = value.shape[:-1]
        value = value.reshape(lead + ((outer, 2) if minor else (2, outer)) + (4, chunk))
        return value if minor else jnp.swapaxes(value, -4, -3)

    def units_of(value, whose):
        value = lax.dynamic_index_in_dim(split_units(value), replica, value.ndim + 1, keepdims=False)
        value = lax.dynamic_index_in_dim(value, whose, value.ndim - 2, keepdims=False)
        return value.reshape(value.shape[:-2] + (wide,))

    def block_index(whose):
        return replica * 2 + whose if minor else whose * 4 + replica

    def heads_of(value, whose):
        lead = value.shape[:-1]
        value = value.reshape(lead + (3, ranks, block))
        value = lax.dynamic_index_in_dim(value, block_index(whose), value.ndim - 2, keepdims=False)
        return value.reshape(lead + (3 * block,))

    def both_sides(own, other):
        return jnp.where(side == 0, jnp.stack([own, other]), jnp.stack([other, own]))

    def gather_rows(value):
        whole = lax.all_gather(value, "fo", axis=0, tiled=False)
        if not minor:
            whole = jnp.swapaxes(whole, 0, 1)
        return whole.reshape(features, value.shape[-1])

    def scatter_outer(partial):
        return lax.psum_scatter(partial, "fo", scatter_dimension=0, tiled=False)

    def scatter_rows(partial):
        partial = partial.reshape(((outer, 2) if minor else (2, outer)) + (rows, partial.shape[-1]))
        if not minor:
            partial = jnp.swapaxes(partial, 0, 1)
        owned = scatter_outer(partial)
        kept = lax.dynamic_index_in_dim(owned, side, 0, keepdims=False)
        given = lax.dynamic_index_in_dim(owned, 1 - side, 0, keepdims=False)
        return both_sides(kept, swap(given, "fi"))

    members = (
        input_norm_gain,
        input_norm_bias,
        post_norm_gain,
        post_norm_bias,
        dense_bias,
        contract_bias,
        query_key_value_bias,
        expand_bias,
    )
    owner = lax.axis_index(fold)
    packed = jnp.concatenate(members)
    packed = lax.dynamic_update_index_in_dim(
        jnp.zeros((owners,) + packed.shape, packed.dtype), packed, owner, 0
    )
    packed = total_over(packed, ("fi", "fo"))
    vectors = []
    offset = 0
    for member in members:
        length = member.shape[0]
        vectors.append(packed[:, offset : offset + length].reshape(-1).astype(jnp.float32))
        offset += length
    (
        first_gain,
        first_shift,
        second_gain,
        second_shift,
        dense_shift,
        shrink_shift,
        joined_shift,
        expand_shift,
    ) = vectors

    masked = jnp.where(valid_mask[:, None] > 0, cotangent, jnp.zeros_like(cotangent))
    hidden = plane_gather(hidden_in)
    expand_own = units_of(expand_weight, side)
    expand_pair = both_sides(expand_own, swap(units_of(expand_weight, 1 - side), "fi"))
    expand = gather_rows(expand_pair)
    shrink_own = lax.dynamic_index_in_dim(
        contract_weight.reshape(4, chunk, features), replica, 0, keepdims=False
    )
    shrink = lax.all_gather(shrink_own, "fo", axis=0, tiled=True)
    joined_own = heads_of(query_key_value_weight, side)
    joined_pair = both_sides(joined_own, swap(heads_of(query_key_value_weight, 1 - side), "fi"))
    joined_weight = gather_rows(joined_pair)
    dense_own = lax.dynamic_index_in_dim(
        dense_weight.reshape(4, rows // 4, features), replica, 0, keepdims=False
    )
    dense_part = lax.all_gather(dense_own, "fo", axis=0, tiled=False)
    group = outer // 4
    dense = replica_exchange(dense_part.reshape(4, group, rows // 4, features))
    dense = jnp.swapaxes(dense, 0, 1).reshape(block, features)
    grad = plane_gather(masked)
    starts = token_starts(segment_ids)
    starts_all = small_gather(starts)
    offsets = jnp.tile(jnp.arange(tokens, dtype=jnp.int32), ranks) - starts_all
    cosine, sine = rotary_tables(offsets)

    normed, _ = normalize(hidden.astype(jnp.float32))
    first_in = (normed * first_gain + first_shift).astype(jnp.bfloat16)
    second_in = (normed * second_gain + second_shift).astype(jnp.bfloat16)

    def product(a, b, left, right):
        return lax.dot_general(a, b, (((left,), (right,)), ((), ())), preferred_element_type=jnp.float32)

    expanded = product(second_in, expand, 1, 0) + units_of(expand_shift, side)
    erf_term = lax.erf(expanded * 0.7071067811865476)
    activated = (0.5 * expanded * (1.0 + erf_term)).astype(jnp.bfloat16)
    feed_part = product(activated, shrink, 1, 0).astype(jnp.bfloat16)
    activated_grad = product(grad, shrink, 1, 1)
    slope = 0.5 * (1.0 + erf_term) + expanded * jnp.exp(-0.5 * expanded * expanded) * 0.3989422804014327
    expand_grad = (activated_grad * slope).astype(jnp.bfloat16)
    shrink_weight_part = product(activated, grad, 0, 0).astype(jnp.bfloat16)
    expand_weight_part = product(second_in, expand_grad, 0, 0).astype(jnp.bfloat16)
    second_grad = product(expand_grad, expand, 1, 1)
    feed = plane_scatter(feed_part.reshape(ranks, tokens, features)) + shrink_shift

    joined = product(first_in, joined_weight, 1, 0) + heads_of(joined_shift, side)
    mixed_grad = product(grad, dense, 1, 1).astype(jnp.bfloat16)
    mixed, joined_grad = attention(joined, mixed_grad, cosine, sine, starts_all[:, None], tokens)
    attention_part = product(mixed, dense, 1, 0).astype(jnp.bfloat16)
    attended = plane_scatter(attention_part.reshape(ranks, tokens, features)) + dense_shift
    dense_weight_part = product(mixed, grad, 0, 0).astype(jnp.bfloat16)
    joined_weight_part = product(first_in, joined_grad, 0, 0).astype(jnp.bfloat16)
    first_grad = product(joined_grad, joined_weight, 1, 1)

    normed_grad_part = (first_grad * first_gain + second_grad * second_gain).astype(jnp.bfloat16)
    normed_grad = plane_scatter(normed_grad_part.reshape(ranks, tokens, features))

    inputs = hidden_in.astype(jnp.float32)
    own_normed, own_inverse = normalize(inputs)
    result = inputs + attended + feed
    hidden_gradient = masked.astype(jnp.float32) + own_inverse * (
        normed_grad
        - jnp.mean(normed_grad, axis=-1, keepdims=True)
        - own_normed * jnp.mean(normed_grad * own_normed, axis=-1, keepdims=True)
    )

    shrink_owned = scatter_outer(shrink_weight_part.reshape(outer, chunk, features))
    shrink_weight_grad = replica_gather(shrink_owned).reshape(contract_weight.shape).astype(jnp.float32)
    expand_owned = replica_gather(scatter_rows(expand_weight_part))
    expand_owned = expand_owned.reshape(4, 2, rows, outer, chunk)
    expand_weight_grad = (
        jnp.transpose(expand_owned, (2, 3, 1, 0, 4) if minor else (2, 1, 3, 0, 4))
        .reshape(rows, units)
        .astype(jnp.float32)
    )
    joined_owned = replica_gather(scatter_rows(joined_weight_part)).reshape(4, 2, rows, 3, block)
    joined_weight_grad = (
        jnp.transpose(joined_owned, (2, 3, 0, 1, 4) if minor else (2, 3, 1, 0, 4))
        .reshape(rows, 3 * features)
        .astype(jnp.float32)
    )
    dense_blocks = jnp.swapaxes(dense_weight_part.reshape(group, 4, rows // 4, features), 0, 1)
    dense_blocks = replica_exchange(dense_blocks).reshape(outer, rows // 4, features)
    dense_owned = scatter_outer(dense_blocks)
    dense_weight_grad = replica_gather(dense_owned).reshape(rows, features).astype(jnp.float32)

    mask_float = valid_mask.astype(jnp.float32)[:, None]
    statistics = jnp.stack(
        [
            jnp.sum(mask_float * inputs * inputs),
            jnp.sum(mask_float * attended * attended),
            jnp.sum(mask_float * feed * feed),
            jnp.sum(mask_float * result * result),
            jnp.sum(mask_float),
        ]
    )
    joined_bias_sum = jnp.sum(joined_grad, axis=0, dtype=jnp.float32).reshape(3, 1, block)
    joined_bias_sum = lax.dynamic_update_slice(
        jnp.zeros((3, ranks, block), jnp.float32), joined_bias_sum, (0, block_index(side), 0)
    )
    expand_bias_sum = jnp.sum(expand_grad, axis=0, dtype=jnp.float32).reshape(outer, 1, 1, chunk)
    expand_bias_sum = lax.dynamic_update_slice(
        jnp.zeros((outer, 2, 4, chunk), jnp.float32), expand_bias_sum, (0, side, replica, 0)
    )
    if not minor:
        expand_bias_sum = jnp.swapaxes(expand_bias_sum, 0, 1)
    summed = total_over(
        jnp.concatenate(
            [
                jnp.sum(first_grad * normed, axis=0),
                jnp.sum(first_grad, axis=0),
                jnp.sum(second_grad * normed, axis=0),
                jnp.sum(second_grad, axis=0),
                jnp.sum(masked.astype(jnp.float32), axis=0),
                joined_bias_sum.reshape(-1),
                expand_bias_sum.reshape(-1),
                statistics,
            ]
        ),
        ("pc", "px", "fi", "fo"),
    )

    def owned_part(start, length):
        return lax.dynamic_slice_in_dim(summed, start + owner * (length // owners), length // owners)

    bias_out = owned_part(4 * features, features)
    final = 8 * features + units
    branch_norms = jnp.sqrt(summed[final : final + 4] / (summed[final + 4] * features))
    return (
        result.astype(jnp.bfloat16),
        hidden_gradient,
        owned_part(0, features),
        owned_part(features, features),
        joined_weight_grad,
        owned_part(5 * features, 3 * features),
        dense_weight_grad,
        bias_out,
        owned_part(2 * features, features),
        owned_part(3 * features, features),
        expand_weight_grad,
        owned_part(8 * features, units),
        shrink_weight_grad,
        bias_out,
        branch_norms,
    )


def solution(mesh):
    owners = mesh.shape["fsdp"]
    replicas = mesh.shape["dp"]
    minor = 2048 // owners >= HEAD
    outer = owners // 2
    names = ("fo", "fi", "px", "pc") if minor else ("fi", "fo", "px", "pc")
    sizes = (outer, 2) if minor else (2, outer)
    split = Mesh(mesh.devices.reshape(sizes + (replicas // 2, 2)), names)
    fsdp = names[:2]
    every = names
    matrix = P(fsdp, None)
    vector = P(fsdp)
    in_specs = (
        P(every, None),
        P(every, None),
        P(every),
        P(every),
        vector,
        vector,
        matrix,
        vector,
        matrix,
        vector,
        vector,
        vector,
        matrix,
        vector,
        matrix,
        vector,
    )
    out_specs = (
        P(every, None),
        P(every, None),
        vector,
        vector,
        matrix,
        vector,
        matrix,
        vector,
        vector,
        vector,
        matrix,
        vector,
        matrix,
        vector,
        P(),
    )

    def layer(*arguments):
        return per_device(minor, *arguments)

    return jax.shard_map(
        layer, mesh=split, in_specs=in_specs, out_specs=out_specs, check_vma=False
    )
```
